32 devices in a mesh: dp: 16 (over z, x, core), tensor: 2 (over y).
Axes of the slice: x: 2, y: 2, z: 4, core: 2. Of those that a mesh axis runs over, the one named last changes fastest.
Arguments:
- query_rows: bfloat16 [6144, 5120], P('dp', 'tensor'), may hold values from -128 to 128
- key_rows: bfloat16 [6144, 5120], P('dp', 'tensor'), may hold values from -5 to 5
- value_rows: bfloat16 [6144, 5120], P('dp', 'tensor'), may hold values from -12 to 12
- action_mask: int32 [16, 384], P('dp'), may hold values from 0 to 1, as said below
- residual: bfloat16 [6144, 5120], P('dp', 'tensor'), may hold values from -100 to 100
- out_weight: bfloat16 [5120, 5120], P(None, 'tensor'), may hold values from -0.078125 to 0.078125
- norm_gain: float32 [5120], P('tensor'), may hold values from 0.1 to 1.9
- upstream: bfloat16 [6144, 5120], P('dp', 'tensor'), may hold values from -6 to 6
- residual_grad: bfloat16 [6144, 5120], P('dp', 'tensor'), may hold values from -2 to 2
Outputs:
- layer_out: bfloat16 [6144, 5120], P('dp', 'tensor')
- grad_residual: bfloat16 [6144, 5120], P('dp', 'tensor')
- grad_query: bfloat16 [6144, 5120], P('dp', 'tensor')
- grad_key: bfloat16 [6144, 5120], P('dp', 'tensor')
- grad_value: bfloat16 [6144, 5120], P('dp', 'tensor')
- grad_out_weight: float32 [5120, 5120], P('dp', 'tensor')
- grad_gain: float32 [5120], P('tensor')
The draws below stay inside these ranges and needn't reach their ends.
Inputs may be any that keep to these rules, and one draw needn't show every extreme that they name: `action_mask`: each row is a run of zeros followed by a run of ones; the ones number 1 to 192.
All inputs are finite; a program needn't handle non-finite values.
Results may differ from the reference program's by a relative error of at most 0.015.
Values may be sent and summed in bfloat16 or wider, within the bound.
No kernel may reach another device: no remote copies, remote signals or barrier semaphores. Data moves between devices by JAX's collectives and lax.ppermute only.
A program may use at most 192 MiB of HBM per device.

```python
import jax
import jax.numpy as jnp
from jax import lax

D = 5120
HEADS = 40
HEAD_DIM = 128
LEN = 384
SEQS = 16
TOKENS = 6144


def attention_inputs(key):
    base_key = jax.random.fold_in(key, 17)
    key_query, key_key = jax.random.split(base_key, 2)
    shape = (SEQS, LEN, HEADS, HEAD_DIM)
    query_draw = jax.random.truncated_normal(key_query, -4.0, 4.0, shape, jnp.float32)
    key_draw = jax.random.truncated_normal(key_key, -4.0, 4.0, shape, jnp.float32)
    width = HEADS * HEAD_DIM
    return (query_draw.reshape(TOKENS, width), key_draw.reshape(TOKENS, width))


def draw_query_rows(key, part):
    return attention_inputs(key)[0].astype(jnp.bfloat16)


def draw_key_rows(key, part):
    return attention_inputs(key)[1].astype(jnp.bfloat16)


def draw_residual(key, part):
    key_base, key_rows = jax.random.split(jax.random.fold_in(key, 29), 2)
    columns = jnp.arange(D).astype(jnp.float32)
    column_scale = 10.0 ** (0.5 * columns / (D - 1))
    row_scale = jnp.exp(jax.random.uniform(key_rows, (TOKENS, 1), jnp.float32, jnp.log(0.5), jnp.log(5.0)))
    base = jax.random.truncated_normal(key_base, -5.0, 5.0, (TOKENS, D), jnp.float32)
    return (base * row_scale * column_scale[None, :]).astype(jnp.bfloat16)


def draw_action_mask(key, part):
    actions = jax.random.randint(jax.random.fold_in(key, 41), (SEQS,), 1, LEN // 2 + 1)
    position = jnp.arange(LEN)
    return (position[None, :] >= LEN - actions[:, None]).astype(jnp.int32)


def spiked(drawn, stream_key, source, target, parts, factor):
    def block_of(dim):
        return (jnp.arange(drawn.shape[dim]) // (drawn.shape[dim] // parts)).reshape((-1,) + (1,) * (drawn.ndim - 1 - dim))

    first = jax.random.permutation(stream_key, parts)[block_of(target)]
    far = (block_of(target) + parts // 2) % parts
    return jnp.where((block_of(source) == first) | (block_of(source) == far), factor * drawn, drawn)


def steps_of(rng, extent, shards, least, high):
    def one(dim, parts):
        heights = jax.random.uniform(jax.random.fold_in(jax.random.fold_in(rng, 6), dim), (parts,), jnp.float32, least / len(shards), high / len(shards))
        return jnp.repeat(jnp.exp(heights), extent[dim] // parts).reshape((-1,) + (1,) * (len(extent) - dim - 1))

    factor_of = one(*shards[0])
    for cut in shards[1:]:
        factor_of = factor_of * one(*cut)
    return factor_of


def centred(own_key, extent, scale, reach, cuts=(), held_as=jnp.bfloat16):
    result = scale * jax.random.normal(own_key, extent, jnp.float32)
    if cuts:
        result = result * steps_of(own_key, extent, cuts, -0.22, 0.18)
    return jnp.clip(result, -reach, reach).astype(held_as)


def gaussian_with(key, shape, scale, most, shards, heavy, kind=jnp.bfloat16):
    drawn = scale * jax.random.normal(key, shape, jnp.float32)
    if shards:
        drawn = drawn * steps_of(key, shape, shards, -0.22, 0.18)
    return jnp.clip(spiked(drawn, jax.random.fold_in(key, 3), *heavy), -most, most).astype(kind)


def setup_inputs(seed: int = 0) -> dict:
    key_of = jax.random.split(jax.random.key(seed), 10)
    return {
        "query_rows": draw_query_rows(jax.random.fold_in(key_of[9], 71), 0),
        "key_rows": draw_key_rows(jax.random.fold_in(key_of[9], 71), 0),
        "value_rows": centred(key_of[2], (TOKENS, HEADS * HEAD_DIM), 2.0, 12.0, ((0, 16), (1, 2))),
        "action_mask": draw_action_mask(jax.random.fold_in(key_of[9], 71), 0),
        "residual": draw_residual(jax.random.fold_in(key_of[9], 71), 0),
        "out_weight": centred(key_of[5], (D, HEADS * HEAD_DIM), (HEADS * HEAD_DIM) ** -0.5, 0.078125, ((1, 2),)),
        "norm_gain": jnp.clip(1.0 + 0.18 * jax.random.normal(key_of[6], (D,), jnp.float32), 0.1, 1.9),
        "upstream": gaussian_with(key_of[7], (TOKENS, D), 1.0, 6.0, ((0, 16), (1, 2)), (0, 1, 16, 2.0)),
        "residual_grad": centred(key_of[8], (TOKENS, D), 0.3, 2.0, ((0, 16), (1, 2))),
    }


epsilon = 1e-05

def visible(mask_row):
    position = jnp.arange(mask_row.shape[0])
    causal = position[None, :] <= position[:, None]
    observe = mask_row == 0
    return causal | observe[:, None] & observe[None, :]

def softmax_rows(query_heads, keyset, allowed):
    scores = jnp.einsum('qhd,khd->hqk', query_heads.astype(jnp.float32), keyset.astype(jnp.float32)) * HEAD_DIM ** (-0.5)
    masked = jnp.where(allowed[None], scores, -jnp.inf)
    row_top = lax.optimization_barrier(jnp.max(masked, axis=-1, keepdims=True))
    weights = jnp.exp(masked - row_top)
    return weights / lax.optimization_barrier(jnp.sum(weights, axis=-1, keepdims=True))

def split_heads(rows):
    return rows.reshape(LEN, HEADS, HEAD_DIM)

def forward_seq(inputs):
    query_seq, key_seq, value_seq, mask_row = inputs
    chances = softmax_rows(split_heads(query_seq), split_heads(key_seq), visible(mask_row))
    chances_low = lax.optimization_barrier(chances.astype(jnp.bfloat16)).astype(jnp.float32)
    attended = jnp.einsum('hqk,khd->qhd', chances_low, split_heads(value_seq).astype(jnp.float32))
    return attended.astype(jnp.bfloat16).reshape(LEN, HEADS * HEAD_DIM)

def backward_seq(inputs):
    query_seq, key_seq, value_seq, mask_row, grad_seq = inputs
    query_heads = split_heads(query_seq)
    key_heads = split_heads(key_seq)
    chances = softmax_rows(query_heads, key_heads, visible(mask_row))
    chances_low = lax.optimization_barrier(chances.astype(jnp.bfloat16)).astype(jnp.float32)
    grad_heads = split_heads(grad_seq).astype(jnp.float32)
    grad_value = jnp.einsum('hqk,qhd->khd', chances_low, grad_heads).astype(jnp.bfloat16)
    grad_chances = jnp.einsum('qhd,khd->hqk', grad_heads, split_heads(value_seq).astype(jnp.float32))
    row_delta = lax.optimization_barrier(jnp.sum(chances * grad_chances, axis=-1, keepdims=True))
    grad_scores = (chances * (grad_chances - row_delta) * HEAD_DIM ** (-0.5)).astype(jnp.bfloat16)
    grad_scores = lax.optimization_barrier(grad_scores).astype(jnp.float32)
    grad_query = jnp.einsum('hqk,khd->qhd', grad_scores, key_heads.astype(jnp.float32)).astype(jnp.bfloat16)
    grad_key = jnp.einsum('hqk,qhd->khd', grad_scores, query_heads.astype(jnp.float32)).astype(jnp.bfloat16)
    width = HEADS * HEAD_DIM
    return (grad_query.reshape(LEN, width), grad_key.reshape(LEN, width), grad_value.reshape(LEN, width))

def reference(query_rows, key_rows, value_rows, action_mask, residual, out_weight, norm_gain, upstream, residual_grad):
    width = HEADS * HEAD_DIM
    query_seq = query_rows.reshape(SEQS, LEN, width)
    key_seq = key_rows.reshape(SEQS, LEN, width)
    value_seq = value_rows.reshape(SEQS, LEN, width)
    attended = lax.map(forward_seq, (query_seq, key_seq, value_seq, action_mask)).reshape(TOKENS, width)
    projected = jnp.dot(attended, out_weight.T, preferred_element_type=jnp.float32)
    layer_out = (projected + residual.astype(jnp.float32)).astype(jnp.bfloat16)
    out_float = layer_out.astype(jnp.float32)
    row_rms = jnp.sqrt(lax.optimization_barrier(jnp.mean(out_float * out_float, axis=1, keepdims=True)) + epsilon)
    normed = out_float / row_rms
    scaled = upstream.astype(jnp.float32) * norm_gain[None, :]
    row_inner = lax.optimization_barrier(jnp.sum(scaled * out_float, axis=1, keepdims=True)) / (row_rms * D)
    grad_residual = (residual_grad.astype(jnp.float32) + (scaled - normed * row_inner) / row_rms).astype(jnp.bfloat16)
    grad_gain = lax.optimization_barrier(jnp.sum(upstream.astype(jnp.float32) * normed, axis=0))
    grad_out_weight = lax.dot_general(grad_residual, attended, (((0,), (0,)), ((), ())), preferred_element_type=jnp.float32)
    grad_attended = jnp.dot(grad_residual, out_weight, preferred_element_type=jnp.float32).astype(jnp.bfloat16)
    grad_seq = grad_attended.reshape(SEQS, LEN, width)
    grad_query, grad_key, grad_value = lax.map(backward_seq, (query_seq, key_seq, value_seq, action_mask, grad_seq))
    return (layer_out, grad_residual, grad_query.reshape(TOKENS, width), grad_key.reshape(TOKENS, width), grad_value.reshape(TOKENS, width), grad_out_weight, grad_gain)
```

```python
import functools

import jax
import jax.numpy as jnp
from jax import lax
from jax.experimental import pallas as pl
from jax.experimental.pallas import tpu as pltpu
from jax.sharding import PartitionSpec as P

HEAD_DIM = 128
EPSILON = 1e-05
CORES = 2


F32 = jnp.float32
BF16 = jnp.bfloat16
NN = (((1,), (0,)), ((), ()))
NT = (((1,), (1,)), ((), ()))
TN = (((0,), (0,)), ((), ()))


def dot(a, b, dims):
    return lax.dot_general(a, b, dims, preferred_element_type=F32)


def block_of(extent, choices):
    for size in choices:
        if extent % size == 0:
            return size
    return extent


def attend_kernel(mask_ref, query_ref, key_ref, value_ref, out_ref):
    length = query_ref.shape[0]
    scores = dot(query_ref[...], key_ref[...], NT) * HEAD_DIM ** (-0.5)
    rows = lax.broadcasted_iota(jnp.int32, (length, length), 0)
    columns = lax.broadcasted_iota(jnp.int32, (length, length), 1)
    allowed = (columns <= rows) | (mask_ref[0] == 0)
    masked = jnp.where(allowed, scores, -jnp.inf)
    weights = jnp.exp(masked - jnp.max(masked, axis=1, keepdims=True))
    chances = weights * (1.0 / jnp.sum(weights, axis=1, keepdims=True))
    out_ref[...] = dot(chances.astype(BF16), value_ref[...], NN).astype(BF16)


def attend(mask, query, key, value):
    seqs, length = mask.shape[0], mask.shape[-1]
    heads = query.shape[1] // HEAD_DIM
    block = pl.BlockSpec((length, HEAD_DIM), lambda s, h: (s, h))
    return pl.pallas_call(
        attend_kernel,
        grid=(seqs, heads),
        in_specs=[pl.BlockSpec((1, 1, length), lambda s, h: (s, 0, 0))] + [block] * 3,
        out_specs=block,
        out_shape=jax.ShapeDtypeStruct(query.shape, BF16),
        compiler_params=pltpu.CompilerParams(dimension_semantics=("arbitrary",) * 2),
        name="attend",
    )(mask, query, key, value)


def attend_grad_kernel(
    mask_ref, query_ref, key_ref, value_ref, grad_ref, gq_ref, gk_ref, gv_ref
):
    length = query_ref.shape[0]
    scale = HEAD_DIM ** (-0.5)
    query, key, value, grad = query_ref[...], key_ref[...], value_ref[...], grad_ref[...]
    scores = dot(key, query, NT) * scale
    keys = lax.broadcasted_iota(jnp.int32, (length, length), 0)
    rows = lax.broadcasted_iota(jnp.int32, (length, length), 1)
    allowed = (keys <= rows) | (mask_ref[0] == 0)
    masked = jnp.where(allowed, scores, -jnp.inf)
    weights = jnp.exp(masked - jnp.max(masked, axis=0, keepdims=True))
    chances = weights * (1.0 / jnp.sum(weights, axis=0, keepdims=True))
    gv_ref[...] = dot(chances.astype(BF16), grad, NN).astype(BF16)
    grad_chances = dot(value, grad, NT)
    delta = jnp.sum(chances * grad_chances, axis=0, keepdims=True)
    grad_scores = (chances * (grad_chances - delta) * scale).astype(BF16)
    gk_ref[...] = dot(grad_scores, query, NN).astype(BF16)
    gq_ref[...] = dot(grad_scores, key, TN).astype(BF16)


def attend_grad(mask, query, key, value, grad):
    seqs, length = mask.shape[0], mask.shape[1]
    heads = query.shape[1] // HEAD_DIM
    block = pl.BlockSpec((length, HEAD_DIM), lambda s, h: (s, h))
    return pl.pallas_call(
        attend_grad_kernel,
        grid=(seqs, heads),
        in_specs=[pl.BlockSpec((1, length, 1), lambda s, h: (s, 0, 0))] + [block] * 4,
        out_specs=[block] * 3,
        out_shape=[jax.ShapeDtypeStruct(query.shape, BF16)] * 3,
        compiler_params=pltpu.CompilerParams(dimension_semantics=("arbitrary",) * 2),
        name="attend_grad",
    )(mask, query, key, value, grad)


def project_kernel(owner_ref, attended_ref, weight_ref, out_ref):
    out_ref[...] = dot(attended_ref[...], weight_ref[...], NT).astype(out_ref.dtype)


def project(owner, attended, weight, width, first, extent, dtype):
    rows, depth = attended.shape
    size = block_of(extent, (640, 512, 256, 128))
    return pl.pallas_call(
        project_kernel,
        grid_spec=pltpu.PrefetchScalarGridSpec(
            num_scalar_prefetch=1,
            grid=(extent // size,),
            in_specs=[
                pl.BlockSpec((rows, depth), lambda i, o: (0, 0)),
                pl.BlockSpec(
                    (size, depth), lambda i, o: (o[0] * (width // size) + first // size + i, 0)
                ),
            ],
            out_specs=pl.BlockSpec((rows, size), lambda i, o: (0, i)),
        ),
        out_shape=jax.ShapeDtypeStruct((rows, extent), dtype),
        name="project",
    )(owner, attended, weight)


def norm_grad_kernel(
    out_ref, upstream_ref, back_ref, gain_ref, rms_ref, inner_ref, grad_ref, turned_ref, sum_ref
):
    inverse = 1.0 / rms_ref[...]
    upstream = upstream_ref[...].astype(F32)
    normed = out_ref[...].astype(F32) * inverse
    scaled = upstream * gain_ref[...]
    grad = back_ref[...].astype(F32) + (scaled - normed * inner_ref[...]) * inverse
    grad_ref[...] = grad.astype(BF16)
    turned_ref[...] = grad.T.astype(BF16)
    sum_ref[...] = jnp.sum(upstream * normed, axis=0, keepdims=True)


def norm_grad(layer_out, upstream, back, gain, rms, inner):
    rows, width = layer_out.shape
    size = block_of(width, (256, 128))
    block = pl.BlockSpec((rows, size), lambda i: (0, i))
    line = pl.BlockSpec((1, size), lambda i: (0, i))
    column = pl.BlockSpec((rows, 1), lambda i: (0, 0))
    return pl.pallas_call(
        norm_grad_kernel,
        grid=(width // size,),
        in_specs=[block, block, block, line, column, column],
        out_specs=[block, pl.BlockSpec((size, rows), lambda i: (i, 0)), line],
        out_shape=[
            jax.ShapeDtypeStruct((rows, width), BF16),
            jax.ShapeDtypeStruct((width, rows), BF16),
            jax.ShapeDtypeStruct((1, width), F32),
        ],
        name="norm_grad",
    )(layer_out, upstream, back, gain, rms, inner)


def back_kernel(owner_ref, turned_ref, weight_ref, *rest, steps):
    before, out_ref, total = rest[:-2], rest[-2], rest[-1]
    step = pl.program_id(0)
    product = dot(turned_ref[...], weight_ref[...], TN)

    @pl.when(step == 0)
    def _():
        total[...] = product + before[0][...] if before else product

    @pl.when(step > 0)
    def _():
        total[...] += product

    @pl.when(step == steps - 1)
    def _():
        out_ref[...] = total[...].astype(out_ref.dtype)


def back_project(owner, turned, weight, before, dtype):
    width, rows = turned.shape
    depth = weight.shape[1]
    size = block_of(width, (640, 512, 256, 128))
    steps = width // size
    whole = pl.BlockSpec((rows, depth), lambda i, o: (0, 0))
    return pl.pallas_call(
        functools.partial(back_kernel, steps=steps),
        grid_spec=pltpu.PrefetchScalarGridSpec(
            num_scalar_prefetch=1,
            grid=(steps,),
            in_specs=[
                pl.BlockSpec((size, rows), lambda i, o: (i, 0)),
                pl.BlockSpec((size, depth), lambda i, o: (o[0] * steps + i, 0)),
            ]
            + [whole] * len(before),
            out_specs=whole,
            scratch_shapes=[pltpu.VMEM((rows, depth), F32)],
        ),
        out_shape=jax.ShapeDtypeStruct((rows, depth), dtype),
        name="back_project",
    )(owner, turned, weight, *before)


def weight_grad_kernel(*refs, count, extra):
    turned, attended = refs[:count], refs[count : 2 * count]
    more, out_ref = refs[2 * count : 2 * count + extra], refs[-1]
    total = dot(turned[0][...], attended[0][...], NN)
    for k in range(1, count):
        total += dot(turned[k][...], attended[k][...], NN)
    for ref in more:
        total += ref[...].astype(F32)
    out_ref[...] = total.astype(out_ref.dtype)


def weight_grad(turned, attended, more, dtype):
    features, rows = turned[0].shape
    depth = attended[0].shape[1]
    size = block_of(depth, (256, 128))
    out = pl.BlockSpec((features, size), lambda i: (0, i))
    return pl.pallas_call(
        functools.partial(weight_grad_kernel, count=len(turned), extra=len(more)),
        grid=(depth // size,),
        in_specs=[pl.BlockSpec((features, rows), lambda i: (0, 0))] * len(turned)
        + [pl.BlockSpec((rows, size), lambda i: (0, i))] * len(attended)
        + [out] * len(more),
        out_specs=out,
        out_shape=jax.ShapeDtypeStruct((features, depth), dtype),
        name="weight_grad",
    )(*turned, *attended, *more)


def shards(
    dp,
    tensor,
    query_rows,
    key_rows,
    value_rows,
    action_mask,
    residual,
    out_weight,
    norm_gain,
    upstream,
    residual_grad,
):
    cores = CORES if dp % CORES == 0 else 1
    rest = dp // cores
    ring = 1
    while ring * ring < rest and rest % (2 * ring) == 0:
        ring *= 2
    near = rest // ring
    me = lax.axis_index("dp")
    mine = lax.axis_index("tensor")
    my_core, my_side, my_ring = me % cores, (me // cores) % near, me // (cores * near)

    def index(at_ring, at_side, at_core):
        return ((at_ring % ring) * near + at_side % near) * cores + at_core % cores

    def move(x, by_ring=0, by_side=0, by_core=0):
        pairs = []
        for i in range(dp):
            c, s, r = i % cores, (i // cores) % near, i // (cores * near)
            pairs.append((i, index(r + by_ring, s + by_side, c + by_core)))
        return lax.ppermute(x, "dp", pairs)

    def turn(x, by):
        return lax.ppermute(x, "tensor", [(i, (i + by) % tensor) for i in range(tensor)])

    def all_sum(x, axis, size):
        step = 1
        while step < size:
            x = x + lax.ppermute(x, axis, [(i, i ^ step) for i in range(size)])
            step *= 2
        return x

    rows, depth = query_rows.shape
    width = residual.shape[1]
    features = width * tensor
    seqs, length = action_mask.shape

    attended = attend(
        action_mask.reshape(seqs, 1, length), query_rows, key_rows, value_rows
    )

    held = {0: attended}
    for step in range(1, ring // 2 + 1):
        if 2 * step == ring:
            if step == 1:
                held[1] = move(attended, by_ring=1)
            else:
                half = depth // 2
                held[step] = jnp.concatenate(
                    [
                        move(held[step - 1][:, :half], by_ring=1),
                        move(held[step + 1][:, half:], by_ring=-1),
                    ],
                    axis=1,
                )
        else:
            held[step] = move(held[step - 1], by_ring=1)
            held[ring - step] = move(held[(ring - step + 1) % ring], by_ring=-1)

    chunks = 2
    part = width // chunks
    arrived = []
    for by in range(1, tensor):
        owner = ((mine + by) % tensor).reshape(1)
        share = [
            turn(project(owner, attended, out_weight, width, k * part, part, BF16), by)
            for k in range(chunks)
        ]
        arrived.append(share)
    own = project(mine.reshape(1), attended, out_weight, width, 0, width, F32)
    total = own + residual.astype(F32)
    for share in arrived:
        total = total + jnp.concatenate(share, axis=1).astype(F32)
    layer_out = total.astype(BF16)
    out_float = layer_out.astype(F32)
    scaled = upstream.astype(F32) * norm_gain[None, :]
    sums = jnp.stack(
        [jnp.sum(out_float * out_float, axis=1), jnp.sum(scaled * out_float, axis=1)]
    )
    sums = all_sum(sums, "tensor", tensor)
    row_rms = jnp.sqrt(sums[0] / features + EPSILON)[:, None]
    row_inner = sums[1][:, None] / (row_rms * features)
    grad_residual, turned, gain_share = norm_grad(
        layer_out, upstream, residual_grad, norm_gain[None, :], row_rms, row_inner
    )
    grad_gain = all_sum(gain_share, "dp", dp)[0]

    shares = [turned] + [turn(turned, by) for by in range(1, tensor)]
    back = back_project(mine.reshape(1), turned, out_weight, (), F32 if tensor > 1 else BF16)
    for by in range(1, tensor):
        owner = ((mine - by) % tensor).reshape(1)
        last = by == tensor - 1
        back = back_project(owner, shares[by], out_weight, (back,), BF16 if last else F32)

    gathered = jnp.zeros((tensor, width, rows), BF16)
    for by in range(tensor):
        gathered = lax.dynamic_update_slice(
            gathered, shares[by][None], ((mine - by) % tensor, 0, 0)
        )
    blocks = gathered.reshape(dp, features // dp, rows)

    attended_at = {}
    for r in range(ring):
        for c in range(cores):
            attended_at[r, c] = held[r] if c == 0 else move(held[r], by_core=c)

    def pieces(side):
        turned_at = []
        for r in range(ring):
            for c in range(cores):
                target = index(my_ring + r, my_side + side, my_core + c)
                block = lax.dynamic_index_in_dim(blocks, target, 0, keepdims=False)
                turned_at.append(move(block, by_ring=r, by_core=c) if r or c else block)
        return turned_at, [attended_at[r, c] for r in range(ring) for c in range(cores)]

    sent = []
    for side in range(1, near):
        sent.append(move(weight_grad(*pieces(side), (), BF16), by_side=side))
    grad_out_weight = weight_grad(*pieces(0), sent, F32)

    grad_query, grad_key, grad_value = attend_grad(
        action_mask.reshape(seqs, length, 1), query_rows, key_rows, value_rows, back
    )
    return (
        layer_out,
        grad_residual,
        grad_query,
        grad_key,
        grad_value,
        grad_out_weight,
        grad_gain,
    )


def solution(mesh):
    split = P("dp", "tensor")
    return jax.shard_map(
        functools.partial(shards, mesh.shape["dp"], mesh.shape["tensor"]),
        mesh=mesh,
        in_specs=(
            split,
            split,
            split,
            P("dp", None),
            split,
            P(None, "tensor"),
            P("tensor"),
            split,
            split,
        ),
        out_specs=(split, split, split, split, split, split, P("tensor")),
        check_vma=False,
    )
```
